32 devices in a mesh: dp: 8 (over y, x, core), tensor: 4 (over z).
Axes of the slice: x: 2, y: 2, z: 4, core: 2. Of those that a mesh axis runs over, the one named last changes fastest.
Arguments:
- grad_out: bfloat16 [2048, 4096], P('dp'), may hold values from -6 to 6
- down_weight: bfloat16 [14336, 4096], P('tensor'), may hold values from -0.046875 to 0.046875
- gate_pre: bfloat16 [2048, 14336], P('dp', 'tensor'), may hold values from -8 to 8
- up_pre: bfloat16 [2048, 14336], P('dp', 'tensor'), may hold values from -6 to 6
Outputs:
- factor: float32 [14336, 14336], P('dp', 'tensor')
- grad_up: bfloat16 [2048, 14336], P('dp', 'tensor')
The draws below stay inside these ranges and needn't reach their ends.
All inputs are finite; a program needn't handle non-finite values.
Results may differ from the reference program's by a relative error of at most 0.0046.
Values may be sent and summed in bfloat16 or wider, within the bound.
A program may use at most 128 MiB of HBM per device.

```python
import jax
import jax.numpy as jnp

D = 4096
FF = 14336
TOKENS = 2048


def steps_of(key, dims, shards, low, largest):
    factor_of = 1.0
    for dim, parts in shards:
        heights = jax.random.uniform(jax.random.fold_in(jax.random.fold_in(key, 6), dim), (parts,), jnp.float32, low / len(shards), largest / len(shards))
        factor_of = factor_of * jnp.repeat(jnp.exp(heights), dims[dim] // parts).reshape((-1,) + (1,) * (len(dims) - 1 - dim))
    return factor_of


def centred(rng, shape, deviation, reach, cuts=(), held_as=jnp.bfloat16):
    array = deviation * jax.random.normal(rng, shape, jnp.float32)
    if cuts:
        array = array * steps_of(rng, shape, cuts, -0.22, 0.18)
    return jnp.clip(array, -reach, reach).astype(held_as)


def setup_inputs(seed: int = 0) -> dict:
    splits = jax.random.split(jax.random.key(seed), 5)
    return {
        "grad_out": centred(splits[0], (TOKENS, D), 1.0, 6.0, ((0, 8),)),
        "down_weight": centred(splits[1], (FF, D), FF ** -0.5, 0.046875, ((0, 4),)),
        "gate_pre": centred(splits[2], (TOKENS, FF), 1.5, 8.0, ((0, 8), (1, 4))),
        "up_pre": centred(splits[3], (TOKENS, FF), 1.0, 6.0, ((0, 8), (1, 4))),
    }


def reference(grad_out, down_weight, gate_pre, up_pre):
    hidden_grad = jnp.dot(grad_out, down_weight.T, preferred_element_type=jnp.float32)
    gate_value = gate_pre.astype(jnp.float32)
    sigmoid_gate = jax.nn.sigmoid(gate_value)
    silu_slope = sigmoid_gate * (1.0 + gate_value * (1.0 - sigmoid_gate))
    grad_gate = (hidden_grad * up_pre.astype(jnp.float32) * silu_slope).astype(jnp.bfloat16)
    grad_up = (hidden_grad * gate_value * sigmoid_gate).astype(jnp.bfloat16)
    factor = jnp.dot(grad_gate.T, grad_gate, preferred_element_type=jnp.float32) / jnp.float32(TOKENS)
    return factor, grad_up
```

```python
import functools

import jax
import jax.numpy as jnp
from jax import lax
from jax.experimental import pallas as pl
from jax.experimental.pallas import tpu as pltpu
from jax.sharding import PartitionSpec as P

MESH = pl.DeviceIdType.MESH
PIECES = 2


def both(*terms):
    out = terms[0]
    for term in terms[1:]:
        out = jnp.logical_and(out, term)
    return out


def gather_kernel(n, m, b_ref, buf, relay, local_sem, buf_sem, row_sem, relay_sem, send_sem):
    r = n // m
    tokens = b_ref.shape[1]
    piece = tokens // PIECES
    d, t = lax.axis_index("dp"), lax.axis_index("tensor")
    p, c = d // r, d % r
    last = m - 1
    sent = []

    def block(slot, source):
        return buf.at[slot, pl.ds(pl.multiple_of(source * tokens, tokens), tokens)]

    def part(slot, source, i):
        return buf.at[slot, pl.ds(pl.multiple_of(source * tokens + i * piece, piece), piece)]

    def send(when, src, dst, sem, dp, tensor):
        copy = pltpu.make_async_remote_copy(
            src_ref=src, dst_ref=dst, send_sem=send_sem.at[len(sent)], recv_sem=sem,
            device_id={"dp": dp, "tensor": tensor}, device_id_type=MESH,
        )
        sent.append((when, copy))

        @pl.when(when)
        def _():
            copy.start()

    def arrive(when, dst, sem):
        copy = pltpu.make_async_remote_copy(
            src_ref=dst, dst_ref=dst, send_sem=send_sem.at[0], recv_sem=sem,
            device_id={"dp": d, "tensor": t}, device_id_type=MESH,
        )

        @pl.when(when)
        def _():
            copy.wait_recv()

    here = d >= 0
    owner = p == t
    up, down = both(owner, t < last), both(owner, t > 0)
    lift, drop = both(p == last, t < last), both(p == 0, t > 0)

    def along_column(source, other, src_of):
        for i in range(PIECES):
            send(both(up, other != last), src_of(i), part(r, source, i), row_sem.at[source, i], d, t + 1)
            send(both(down, other != 0), src_of(i), part(r, source, i), row_sem.at[source, i], d, t - 1)

    for i in range(r):
        k = (c + i) % r
        send(lift, b_ref.at[k], relay.at[t, k], relay_sem.at[t, k], d, t + 1)
        send(drop, b_ref.at[k], relay.at[t, k], relay_sem.at[t, k], d, t - 1)
    along_column(d, p, lambda i: b_ref.at[c, pl.ds(i * piece, piece)])
    for i in range(1, r):
        c2 = (c + i) % r
        for k2 in range(r):
            k = (c2 + k2) % r
            send(here, b_ref.at[k], block(k, d), buf_sem.at[k, d], p * r + c2, t)
    xor = m & (m - 1) == 0
    tree = m == 4

    def partner(j):
        return p ^ j if xor else (p + j) % m

    def back(j):
        return p ^ j if xor else (p + m - j) % m

    for i in range(r):
        k = (c + i) % r
        for j in (1, 2) if tree else range(1, m):
            send(here, b_ref.at[k], block(k, d), buf_sem.at[k, d], partner(j) * r + k, t)
    own = pltpu.make_async_copy(b_ref, buf.at[pl.ds(0, r), pl.ds(pl.multiple_of(d * tokens, tokens), tokens)], local_sem)
    own.start()

    def share(source):
        for i in range(1, r):
            c2 = (c + i) % r
            send(here, block(c, source), block(c, source), buf_sem.at[c, source], p * r + c2, t)

    def column_event(j, e):
        other = back(j)
        source = other * r + (c + e) % r
        arrive(here, block(c, source), buf_sem.at[c, source])
        along_column(source, other, lambda i: part(c, source, i))
        if tree and j == 1:
            send(c % 2 == 0, block(c, source), block(c, source), buf_sem.at[c, source], (p ^ 2) * r + c, t)
        if tree and j == 2:
            send(c % 2 == 1, block(c, source), block(c, source), buf_sem.at[c, source], (p ^ 1) * r + c, t)
        share(source)

    def row_event(source, other):
        rise, fall = both(t > p, other != last), both(t < p, other != 0)
        for i in range(PIECES):
            at = part(r, source, i)
            arrive(jnp.logical_or(rise, fall), at, row_sem.at[source, i])
            send(both(rise, t < last), at, at, row_sem.at[source, i], d, t + 1)
            send(both(fall, t > 0), at, at, row_sem.at[source, i], d, t - 1)

    def relay_event(hops, e):
        for helper, step in ((last, -1), (0, 1)):
            origin = t + step * hops
            there = both(p == helper, origin >= 0, origin < m)
            slot = jnp.clip(origin, 0, last)
            k = (c + e) % r
            at = relay.at[slot, k]
            arrive(there, at, relay_sem.at[slot, k])
            send(both(there, t - step >= 0, t - step < m), at, at, relay_sem.at[slot, k], d, t - step)
            send(there, at, block(r, d), row_sem.at[d, 0], slot * r + k, t)

    def partner_event():
        for i in range(1, r):
            source = p * r + (c + i) % r
            arrive(here, block(c, source), buf_sem.at[c, source])
            along_column(source, p, lambda i: part(c, source, i))

    partner_event()
    row_event(d, p)
    column_event(1, 0)
    if m > 2:
        column_event(2, 0)
    relay_event(1, 0)
    for e in range(1, r):
        row_event(p * r + (c + e) % r, p)
        column_event(1, e)
        if m > 2:
            column_event(2, e)
        relay_event(1, e)
    for j in range(1, m):
        for e in range(r):
            if j + 2 < m:
                column_event(j + 2, e)
            other = back(j)
            row_event(other * r + (c + e) % r, other)
            if j + 1 < m:
                relay_event(j + 1, e)

    for e in range(r):
        for helper, when in ((last, t > p), (0, t < p)):
            source = helper * r + e
            arrive(when, block(r, source), row_sem.at[source, 0])
    for i in range(1, r):
        k = (c + i) % r
        for source in range(n):
            arrive(d != source, block(k, source), buf_sem.at[k, source])
    own.wait()
    for when, copy in sent:
        @pl.when(when)
        def _():
            copy.wait_send()


def gather(blocks, n, m):
    r, tokens, width = blocks.shape
    return pl.pallas_call(
        functools.partial(gather_kernel, n, m),
        out_shape=(
            jax.ShapeDtypeStruct((r + 1, n * tokens, width), blocks.dtype),
            jax.ShapeDtypeStruct((m, r, tokens, width), blocks.dtype),
        ),
        in_specs=[pl.BlockSpec(memory_space=pltpu.VMEM)],
        out_specs=(pl.BlockSpec(memory_space=pl.ANY), pl.BlockSpec(memory_space=pl.ANY)),
        scratch_shapes=[
            pltpu.SemaphoreType.DMA,
            pltpu.SemaphoreType.DMA((r, n)),
            pltpu.SemaphoreType.DMA((n, PIECES)),
            pltpu.SemaphoreType.DMA((m, r)),
            pltpu.SemaphoreType.DMA((SENDS[(n, m)],)),
        ],
        compiler_params=pltpu.CompilerParams(has_side_effects=True),
    )(blocks)


def gate_kernel(out_ref, weight_ref, gate_ref, up_ref, grad_gate_ref, grad_up_ref):
    hidden_grad = lax.dot_general(
        out_ref[...], weight_ref[...], (((1,), (1,)), ((), ())), preferred_element_type=jnp.float32
    )
    gate_value = gate_ref[...].astype(jnp.float32)
    sigmoid_gate = jax.nn.sigmoid(gate_value)
    silu_slope = sigmoid_gate * (1.0 + gate_value * (1.0 - sigmoid_gate))
    grad_gate_ref[0] = (hidden_grad * up_ref[...].astype(jnp.float32) * silu_slope).astype(jnp.bfloat16)
    grad_up_ref[...] = (hidden_grad * gate_value * sigmoid_gate).astype(jnp.bfloat16)


def tile_of(width, most):
    return max(size for size in range(128, most + 1, 128) if width % size == 0)


def gate(grad_out, down_weight, gate_pre, up_pre, r):
    tokens, depth = grad_out.shape
    columns = down_weight.shape[0]
    width = columns // r
    tile = tile_of(width, 256)
    per = width // tile
    flat = pl.BlockSpec((tokens, tile), lambda j: (0, j))
    return pl.pallas_call(
        gate_kernel,
        grid=(columns // tile,),
        out_shape=(
            jax.ShapeDtypeStruct((r, tokens, width), jnp.bfloat16),
            jax.ShapeDtypeStruct((tokens, columns), jnp.bfloat16),
        ),
        in_specs=[
            pl.BlockSpec((tokens, depth), lambda j: (0, 0)),
            pl.BlockSpec((tile, depth), lambda j: (j, 0)),
            flat,
            flat,
        ],
        out_specs=(pl.BlockSpec((1, tokens, tile), lambda j: (j // per, 0, j % per)), flat),
        compiler_params=pltpu.CompilerParams(vmem_limit_bytes=40 * 2**20),
    )(grad_out, down_weight, gate_pre, up_pre)


def factor_kernel(scale, slot_ref, rows_ref, columns_ref, out_ref):
    out_ref[...] = scale * lax.dot_general(
        rows_ref[0], columns_ref[0], (((0,), (0,)), ((), ())), preferred_element_type=jnp.float32
    )


def factor_of(buf, slot):
    r, total, width = buf.shape
    r -= 1
    tall, wide = tile_of(width, 256), tile_of(width, 896)
    per = width // wide
    return pl.pallas_call(
        functools.partial(factor_kernel, 1.0 / total),
        out_shape=jax.ShapeDtypeStruct((width, r * width), jnp.float32),
        grid_spec=pltpu.PrefetchScalarGridSpec(
            num_scalar_prefetch=1,
            grid=(r * per, width // tall),
            in_specs=[
                pl.BlockSpec((1, total, tall), lambda j, i, slot: (slot[0], 0, i)),
                pl.BlockSpec((1, total, wide), lambda j, i, slot: (j // per, 0, j % per)),
            ],
            out_specs=pl.BlockSpec((tall, wide), lambda j, i, slot: (i, j)),
        ),
        compiler_params=pltpu.CompilerParams(vmem_limit_bytes=40 * 2**20),
    )(slot, buf, buf)


def count(n, m):
    r = n // m
    tree = m == 4
    total = 2 * r + 2 * PIECES * r + (r - 1) * r + r * (2 if tree else m - 1)
    total += (m - 1) * r * (2 * PIECES + r - 1) + (2 * r if tree else 0)
    return total + n * PIECES * 2 + (m - 1) * r * 4


SENDS = {}


def solution(mesh):
    n, m = mesh.shape["dp"], mesh.shape["tensor"]
    assert n % m == 0 and m > 1
    r = n // m
    SENDS[(n, m)] = count(n, m)

    def local(grad_out, down_weight, gate_pre, up_pre):
        blocks, grad_up = gate(grad_out, down_weight, gate_pre, up_pre, r)
        buf, _ = gather(blocks, n, m)
        d, t = lax.axis_index("dp"), lax.axis_index("tensor")
        slot = jnp.where(d // r == t, d % r, r)
        factor = factor_of(buf, slot.astype(jnp.int32).reshape(1))
        return (factor, grad_up)

    return jax.shard_map(
        local,
        mesh=mesh,
        in_specs=(P("dp", None), P("tensor", None), P("dp", "tensor"), P("dp", "tensor")),
        out_specs=(P("dp", "tensor"), P("dp", "tensor")),
        check_vma=False,
    )
```
